1024 devices in a mesh: slab: 16 (over z), swap: 64 (over x, y, core).
Axes of the slice: x: 4, y: 8, z: 16, core: 2. Of those that a mesh axis runs over, the one named last changes fastest.
Arguments:
- fluid_state: float32 [2, 4096, 128, 256], P(None, ('slab', 'swap')), may hold values from -0.45 to 1.6, as said below
- material: int32 [4096, 128, 256], P(('slab', 'swap')), may hold values from 0 to 7
- table_colour: float32 [3, 8], replicated, may hold values from 0.2 to 2
- table_extinction: float32 [8], replicated, may hold values from 0.2 to 1.5
Outputs:
- new_density: float32 [4096, 128, 256], P(('slab', 'swap'))
- rendered: float32 [4, 32768], P(None, 'swap')
The draws below stay inside these ranges and needn't reach their ends.
Inputs may be any that keep to these rules, and one draw needn't show every extreme that they name: fluid_state[0] is the density, between 0.6 and 1.6; fluid_state[1] is the momentum along the view axis, between -0.45 and 0.45.
All inputs are finite; a program needn't handle non-finite values.
Results may differ from the reference program's by a relative error of at most 0.0003.
Values sent between devices are 32-bit elements; how exact they have to be, the bound alone decides.
A program may use at most 32 MiB of HBM per device.

```python
import math
import jax
import jax.numpy as jnp

NX = 128
NY = 256
MATERIALS = 8
NZ = 4096


def draw_fluid_state(key, part):
    first_key, second_key = jax.random.split(jax.random.fold_in(key, 11))
    extent = (NZ, NX, NY)
    density = jnp.exp(jax.random.uniform(first_key, extent, jnp.float32, math.log(0.6), math.log(1.6)))
    momentum = jax.random.uniform(second_key, extent, jnp.float32, -0.45, 0.45)
    return jnp.stack([density, momentum]).astype(jnp.float32)


def place_ends(array, key, low, top_value):
    shape = array.shape
    place = [jax.random.randint(jax.random.fold_in(key, axis), (), 0, shape[axis]) for axis in range(len(shape))]
    array = array.at[tuple(place)].set(low)
    longest = shape.index(max(shape))
    place[longest] = (place[longest] + 1) % shape[longest]
    return array.at[tuple(place)].set(top_value)


def setup_inputs(seed: int = 0) -> dict:
    splits = jax.random.split(jax.random.key(seed), 5)
    return {
        "fluid_state": draw_fluid_state(jax.random.fold_in(splits[4], 71), 0),
        "material": place_ends(jax.random.randint(splits[1], (NZ, NX, NY), 0, MATERIALS), jax.random.fold_in(splits[1], 1), 0, MATERIALS - 1).astype(jnp.int32),
        "table_colour": jnp.clip(jax.random.uniform(splits[2], (3, MATERIALS), jnp.float32, 0.2, 2.0), 0.2, 2.0),
        "table_extinction": jnp.clip(jnp.exp(jax.random.uniform(splits[3], (MATERIALS,), jnp.float32, math.log(0.2), math.log(1.5))), 0.2, 1.5),
    }


COURANT = 0.4
DEPTH_SCALE = 2.5


def hydro_step(fields):
    density = fields[0]
    momentum = fields[1]
    velocity = momentum / density
    speeds = jnp.abs(velocity) + 1.0
    fluxes = jnp.stack([momentum, momentum * velocity + density])
    face_speed = jnp.maximum(speeds[:-1], speeds[1:])
    face_flux = 0.5 * (fluxes[:, :-1] + fluxes[:, 1:]) - 0.5 * face_speed * (fields[:, 1:] - fields[:, :-1])
    return fields[:, 1:-1] - COURANT * (face_flux[:, 1:] - face_flux[:, :-1])


def reference(fluid_state, material, table_colour, table_extinction):
    fields = fluid_state
    for number in range(4):
        padded = jnp.concatenate([fields[:, -1:], fields, fields[:, :1]], axis=1)
        fields = hydro_step(padded)
    density = fields[0]
    extinction = jnp.zeros(density.shape, jnp.float32)
    for number in range(MATERIALS):
        extinction = extinction + jnp.where(material == number, table_extinction[number], 0.0)
    optical = DEPTH_SCALE * extinction * density / NZ
    running = jnp.cumsum(optical, axis=0)
    weight = jnp.exp(optical - running) * (1.0 - jnp.exp(-optical))
    colour = jnp.zeros((3, NX, NY), jnp.float32)
    for number in range(MATERIALS):
        summed = jnp.sum(jnp.where(material == number, weight, 0.0), axis=0)
        colour = colour + table_colour[:, number][:, None, None] * summed[None]
    opacity = 1.0 - jnp.exp(-running[-1])
    rendered = jnp.concatenate([colour, opacity[None]], axis=0).reshape(4, NX * NY)
    return density, rendered
```

```python
import functools

import jax
import jax.numpy as jnp
from jax import lax
from jax.experimental import pallas as pl
from jax.experimental.pallas import tpu as pltpu
from jax.sharding import PartitionSpec as P

MESH = pl.DeviceIdType.MESH
COURANT = 0.4
DEPTH_SCALE = 2.5
STEPS = 4
LANES = 128
XS = 4
AHEAD = 8
LAG_Y = 8
LAG_X = 1


def sweep_step(rho, mom, last):
    count = len(rho)
    vel = [m / r for m, r in zip(mom, rho)]
    speed = [jnp.abs(v) for v in vel]
    flux = [m * v + r for m, v, r in zip(mom, vel, rho)]
    face_rho, face_mom = [], []
    for i in range(count - 1):
        a = jnp.maximum(speed[i], speed[i + 1]) + 1.0
        face_rho.append((mom[i] + mom[i + 1]) - a * (rho[i + 1] - rho[i]))
        if not last:
            face_mom.append((flux[i] + flux[i + 1]) - a * (mom[i + 1] - mom[i]))
    half = 0.5 * COURANT
    new_rho = [rho[i] - half * (face_rho[i] - face_rho[i - 1]) for i in range(1, count - 1)]
    new_mom = None
    if not last:
        new_mom = [mom[i] - half * (face_mom[i] - face_mom[i - 1]) for i in range(1, count - 1)]
    return new_rho, new_mom


def choose(bits, values):
    level = list(values)
    for bit in bits:
        level = [jnp.where(bit, level[2 * i + 1], level[2 * i]) for i in range(len(level) // 2)]
    return level[0]


def through_everywhere(tile, sub):
    axis = tile.ndim - 2
    only = jnp.where(sub >= 6, tile, 0.0)
    only = only + pltpu.roll(only, 4, axis)
    return only + pltpu.roll(only, 2, axis)


def over(tiles, sub):
    through = [through_everywhere(t, sub) for t in tiles]
    total = tiles[0]
    before = through[0]
    for tile, t in zip(tiles[1:], through[1:]):
        total = total + before * tile
        before = before * t
    return jnp.where(sub < 6, total, before)


def kernel(
    sizes, fluid, material, tcol, text, dens_out, image,
    own, low, high, mat, dens, part, crecv, ysrc, ybuf, xsrc, xbuf, zsrc, zbuf,
    own_sem, mat_sem, low_recv, high_recv, next_send, prev_send,
    core_send, core_recv, y_send, y_recv, x_send, x_recv, z_send, z_recv, dens_sem,
):
    zs, xs, ys = sizes
    halves = 2
    chunks = halves * xs
    layers = fluid.shape[1]
    rows = 4 * ys
    slab = lax.axis_index("slab")
    swap = lax.axis_index("swap")
    members = 2 * xs * ys
    x = swap // (2 * ys)
    y = (swap // 2) % ys
    k = swap % 2

    def member(xx, yy, kk):
        return (xx * ys + yy) * 2 + kk

    place = slab * members + swap
    after = (place + 1) % (zs * members)
    ahead = (place + zs * members - 1) % (zs * members)
    next_id = (after // members, after % members)
    prev_id = (ahead // members, ahead % members)
    partner = (slab, member(x, y, 1 - k))

    def window(ref, c):
        r = pl.multiple_of((c % xs) * rows, rows)
        col = pl.multiple_of((c // xs) * LANES, LANES)
        where = (pl.ds(r, rows), pl.ds(col, LANES))
        lead = (slice(None),) * (len(ref.shape) - 2)
        return ref.at[lead + where]

    def own_copy(c):
        return pltpu.make_async_copy(window(fluid, c), window(own, c), own_sem.at[c])

    def mat_copy(c):
        return pltpu.make_async_copy(window(material, c), window(mat, c), mat_sem.at[c])

    def dens_copy(c):
        return pltpu.make_async_copy(window(dens, c), window(dens_out, c), dens_sem.at[c])

    def remote(src, dst, send, recv, where):
        return pltpu.make_async_remote_copy(
            src_ref=src, dst_ref=dst, send_sem=send, recv_sem=recv, device_id=where, device_id_type=MESH
        )

    def to_next(c):
        return remote(window(own, c), window(low, c), next_send.at[c], low_recv.at[c], next_id)

    def to_prev(c):
        return remote(window(own, c), window(high, c), prev_send.at[c], high_recv.at[c], prev_id)

    def to_core(c):
        return remote(part.at[c, 1 - k], crecv.at[c], core_send.at[c], core_recv.at[c], partner)

    def looped(lo, hi):
        def wrap(body):
            lax.fori_loop(lo, hi, lambda i, _: (body(i), 0)[1], 0)
        return wrap

    @looped(0, chunks)
    def _(c):
        own_copy(c).start()

    @looped(0, chunks)
    def _(c):
        mat_copy(c).start()

    barrier = pltpu.get_barrier_semaphore()

    def greet(where):
        pl.semaphore_signal(barrier, inc=1, device_id=where, device_id_type=MESH)

    greet(next_id)
    greet(prev_id)
    for j in range(1, ys):
        greet((slab, member(x, (y + j) % ys, k)))
    for j in range(1, xs):
        greet((slab, member((x + j) % xs, y, k)))
    for j in range(1, zs):
        greet(((slab + j) % zs, swap))
    pl.semaphore_wait(barrier, 2 + (ys - 1) + (xs - 1) + (zs - 1))

    def send_halo(c):
        own_copy(c).wait()
        to_next(c).start()
        to_prev(c).start()

    looped(0, min(AHEAD, chunks))(send_halo)

    sub = lax.broadcasted_iota(jnp.int32, (8, LANES), 0)
    sub3 = lax.broadcasted_iota(jnp.int32, (ys, 8, LANES), 1)
    ext = [text[n] * (DEPTH_SCALE / (layers * zs * members)) for n in range(8)]
    colour = [[tcol[ch, n] for n in range(8)] for ch in range(3)]

    def compute(c):
        r0 = (c % xs) * rows
        col = pl.multiple_of((c // xs) * LANES, LANES)

        @looped(0, ys // 2)
        def _(yh):
            at = (pl.ds(pl.multiple_of(r0 + yh * 8, 8), 8), pl.ds(col, LANES))
            rho = [r[(0, i) + at] for r in (low, own, high) for i in range(layers)]
            mom = [r[(1, i) + at] for r in (low, own, high) for i in range(layers)]
            for step in range(STEPS):
                rho, mom = sweep_step(rho, mom, step == STEPS - 1)
            before = None
            total = [None] * 3
            for i in range(layers):
                dens[(i,) + at] = rho[i]
                m = mat[(i,) + at]
                bits = [(m & b) != 0 for b in (1, 2, 4)]
                through = jnp.exp(-(choose(bits, ext) * rho[i]))
                weight = 1.0 - through
                if before is not None:
                    weight = before * weight
                before = through if before is None else before * through
                for ch in range(3):
                    term = weight * choose(bits, colour[ch])
                    total[ch] = term if total[ch] is None else total[ch] + term
            a = total + [before]
            top = sub < 4
            b = [None] * 4
            for p in range(2):
                b[p] = jnp.where(top, a[p], pltpu.roll(a[p + 2], 4, 0))
                b[p + 2] = jnp.where(top, pltpu.roll(a[p], 4, 0), a[p + 2])
            even = (sub & 2) == 0
            for q in range(2):
                first, second = b[2 * q], b[2 * q + 1]
                part[c, 0, yh * 2 + q] = jnp.where(even, first, pltpu.roll(second, 2, 0))
                part[c, 1, yh * 2 + q] = jnp.where(even, pltpu.roll(first, 6, 0), second)

    def y_copy(c, j):
        other = (y + j) % ys
        return remote(ysrc.at[c, other], ybuf.at[c, y], y_send.at[c], y_recv.at[c], (slab, member(x, other, k)))

    def x_copy(c):
        return remote(xsrc.at[c], xbuf.at[c // xs, x], x_send.at[c], x_recv.at[c // xs], (slab, member(c % xs, y, k)))

    def z_copy(h, j):
        other = (slab + j) % zs
        return remote(zsrc.at[h], zbuf.at[h, slab], z_send.at[h], z_recv.at[h], (other, swap))

    def arrived(ref, sem):
        pltpu.make_async_copy(ref, ref, sem).wait()

    def first_stage(c):
        low_wait = pltpu.make_async_copy(window(low, c), window(low, c), low_recv.at[c])
        low_wait.wait()
        high_wait = pltpu.make_async_copy(window(high, c), window(high, c), high_recv.at[c])
        high_wait.wait()
        mat_copy(c).wait()
        compute(c)
        to_core(c).start()
        dens_copy(c).start()

    def core_stage(c):
        to_core(c).wait_recv()
        mine, theirs = part[c, k], crecv[c]
        is_first = k == 0
        front = jnp.where(is_first, mine, theirs)
        back = jnp.where(is_first, theirs, mine)
        both = over([front, back], sub3)
        ysrc[c] = both
        ybuf[c, y] = ysrc[c, y]
        for j in range(1, ys):
            y_copy(c, j).start()

    def y_stage(c):
        arrived(ybuf.at[c, pl.ds(0, ys - 1)], y_recv.at[c])
        done = over([ybuf[c, i] for i in range(ys)], sub)

        @pl.when(x == c % xs)
        def _():
            xbuf[c // xs, x] = done

        @pl.when(x != c % xs)
        def _():
            xsrc[c] = done
            x_copy(c).start()

    def x_stage(h):
        arrived(xbuf.at[h, pl.ds(0, xs - 1)], x_recv.at[h])
        done = over([xbuf[h, i] for i in range(xs)], sub)
        zsrc[h] = done
        zbuf[h, slab] = done
        for j in range(1, zs):
            z_copy(h, j).start()

    def z_stage(h):
        arrived(zbuf.at[h, pl.ds(0, zs - 1)], z_recv.at[h])
        done = over([zbuf[h, i] for i in range(zs)], sub)
        image[h] = jnp.where(sub < 6, done, 1.0 - done)

    @looped(0, chunks + 1 + LAG_Y + LAG_X)
    def _(t):
        @pl.when(t < chunks)
        def _():
            first_stage(t)

        if AHEAD < chunks:
            @pl.when(t + AHEAD < chunks)
            def _():
                send_halo(t + AHEAD)

        @pl.when((t >= 1) & (t < chunks + 1))
        def _():
            core_stage(t - 1)

        ty = t - 1 - LAG_Y

        @pl.when((ty >= 0) & (ty < chunks))
        def _():
            y_stage(ty)

        tx = ty - LAG_X

        @pl.when((tx >= 0) & (tx < chunks) & (x == tx % xs))
        def _():
            x_stage(tx // xs)

    for h in range(halves):
        z_stage(h)

    @looped(0, chunks)
    def _(c):
        to_next(c).wait_send()
        to_prev(c).wait_send()
        to_core(c).wait_send()
        arrived(ybuf.at[c, pl.ds(0, ys - 1)], y_send.at[c])

        @pl.when(x != c % xs)
        def _():
            x_copy(c).wait_send()

        dens_copy(c).wait()

    for h in range(halves):
        arrived(zbuf.at[h, pl.ds(0, zs - 1)], z_send.at[h])


def per_device(sizes, fluid_state, material, table_colour, table_extinction):
    zs, xs, ys = sizes
    _, layers, height, width = fluid_state.shape
    chunks = 2 * xs
    f32 = jnp.float32
    dma = pltpu.SemaphoreType.DMA
    hbm = pl.BlockSpec(memory_space=pltpu.HBM)
    vmem = pl.BlockSpec(memory_space=pltpu.VMEM)
    density, image = pl.pallas_call(
        functools.partial(kernel, sizes),
        out_shape=(
            jax.ShapeDtypeStruct((layers, height, width), f32),
            jax.ShapeDtypeStruct((2, 8, LANES), f32),
        ),
        in_specs=[hbm, hbm, pl.BlockSpec(memory_space=pltpu.SMEM), pl.BlockSpec(memory_space=pltpu.SMEM)],
        out_specs=(hbm, vmem),
        scratch_shapes=[
            pltpu.VMEM(fluid_state.shape, f32),
            pltpu.VMEM(fluid_state.shape, f32),
            pltpu.VMEM(fluid_state.shape, f32),
            pltpu.VMEM(material.shape, jnp.int32),
            pltpu.VMEM(material.shape, f32),
            pltpu.VMEM((chunks, 2, ys, 8, LANES), f32),
            pltpu.VMEM((chunks, ys, 8, LANES), f32),
            pltpu.VMEM((chunks, ys, 8, LANES), f32),
            pltpu.VMEM((chunks, ys, 8, LANES), f32),
            pltpu.VMEM((chunks, 8, LANES), f32),
            pltpu.VMEM((2, xs, 8, LANES), f32),
            pltpu.VMEM((2, 8, LANES), f32),
            pltpu.VMEM((2, zs, 8, LANES), f32),
        ]
        + [dma((chunks,))] * 11
        + [dma((2,)), dma((2,)), dma((2,)), dma((chunks,))],
        compiler_params=pltpu.CompilerParams(
            collective_id=0, has_side_effects=True, vmem_limit_bytes=65400000
        ),
        name="sweep_render",
    )(fluid_state, material, table_colour, table_extinction)
    rendered = image.reshape(2, 4, 2, LANES).transpose(1, 2, 0, 3).reshape(4, 4 * LANES)
    return density, rendered


def solution(mesh):
    slabs, members = mesh.shape["slab"], mesh.shape["swap"]
    sizes = (slabs, XS, members // (2 * XS))
    return jax.shard_map(
        functools.partial(per_device, sizes),
        mesh=mesh,
        in_specs=(P(None, ("slab", "swap"), None, None), P(("slab", "swap"), None, None), P(), P()),
        out_specs=(P(("slab", "swap"), None, None), P(None, "swap")),
        check_vma=False,
    )
```

```python
import functools

import jax
import jax.numpy as jnp
from jax import lax
from jax.experimental import pallas as pl
from jax.experimental.pallas import tpu as pltpu
from jax.sharding import PartitionSpec as P

MESH = pl.DeviceIdType.MESH
COURANT = 0.4
DEPTH_SCALE = 2.5
STEPS = 4
LANES = 128
XS = 4
AHEAD = 8
LAG_Y = 8
LAG_X = 4
LAG_C = 1


def sweep_step(rho, mom, last):
    count = len(rho)
    vel = [m / r for m, r in zip(mom, rho)]
    speed = [jnp.abs(v) for v in vel]
    flux = [m * v + r for m, v, r in zip(mom, vel, rho)]
    face_rho, face_mom = [], []
    for i in range(count - 1):
        a = jnp.maximum(speed[i], speed[i + 1]) + 1.0
        face_rho.append((mom[i] + mom[i + 1]) - a * (rho[i + 1] - rho[i]))
        if not last:
            face_mom.append((flux[i] + flux[i + 1]) - a * (mom[i + 1] - mom[i]))
    half = 0.5 * COURANT
    new_rho = [rho[i] - half * (face_rho[i] - face_rho[i - 1]) for i in range(1, count - 1)]
    new_mom = None
    if not last:
        new_mom = [mom[i] - half * (face_mom[i] - face_mom[i - 1]) for i in range(1, count - 1)]
    return new_rho, new_mom


def choose(bits, values):
    level = list(values)
    for bit in bits:
        level = [jnp.where(bit, level[2 * i + 1], level[2 * i]) for i in range(len(level) // 2)]
    return level[0]


def through_everywhere(tile, sub):
    axis = tile.ndim - 2
    only = jnp.where(sub >= 6, tile, 0.0)
    only = only + pltpu.roll(only, 4, axis)
    return only + pltpu.roll(only, 2, axis)


def over(tiles, sub):
    through = [through_everywhere(t, sub) for t in tiles]
    total = tiles[0]
    before = through[0]
    for tile, t in zip(tiles[1:], through[1:]):
        total = total + before * tile
        before = before * t
    return jnp.where(sub < 6, total, before)


def kernel(
    sizes, fluid, material, tcol_hbm, text_hbm, dens, image,
    own, low, high, mat, tcol, text, part, crecv, ysrc, ybuf, xsrc, xbuf, zsrc, zbuf,
    own_sem, mat_sem, low_recv, high_recv, next_send, prev_send,
    core_send, core_recv, y_send, y_recv, x_send, x_recv, z_send, z_recv, table_sem, known,
):
    zs, xs, ys = sizes
    halves = 2
    chunks = halves * xs
    layers = fluid.shape[1]
    rows = 4 * ys
    slab = lax.axis_index("slab")
    swap = lax.axis_index("swap")
    members = 2 * xs * ys
    x = swap // (2 * ys)
    y = (swap // 2) % ys
    k = swap % 2

    def member(xx, yy, kk):
        return (xx * ys + yy) * 2 + kk

    place = slab * members + swap
    after = (place + 1) % (zs * members)
    ahead = (place + zs * members - 1) % (zs * members)
    next_id = (after // members, after % members)
    prev_id = (ahead // members, ahead % members)
    partner = (slab, member(x, y, 1 - k))

    def window(ref, c):
        r = pl.multiple_of((c % xs) * rows, rows)
        col = pl.multiple_of((c // xs) * LANES, LANES)
        where = (pl.ds(r, rows), pl.ds(col, LANES))
        lead = (slice(None),) * (len(ref.shape) - 2)
        return ref.at[lead + where]

    def own_copy(c):
        return pltpu.make_async_copy(window(fluid, c), window(own, c), own_sem.at[c])

    def mat_copy(c):
        return pltpu.make_async_copy(window(material, c), window(mat, c), mat_sem.at[c])

    def remote(src, dst, send, recv, where):
        return pltpu.make_async_remote_copy(
            src_ref=src, dst_ref=dst, send_sem=send, recv_sem=recv, device_id=where, device_id_type=MESH
        )

    def to_next(c):
        return remote(window(own, c), window(low, c), next_send.at[c], low_recv.at[c], next_id)

    def to_prev(c):
        return remote(window(own, c), window(high, c), prev_send.at[c], high_recv.at[c], prev_id)

    def to_core(c):
        return remote(part.at[c, 1 - k], crecv.at[c], core_send.at[c], core_recv.at[c], partner)

    def looped(lo, hi):
        def wrap(body):
            lax.fori_loop(lo, hi, lambda i, _: (body(i), 0)[1], 0)
        return wrap

    @looped(0, chunks)
    def _(c):
        own_copy(c).start()

    @looped(0, chunks)
    def _(c):
        mat_copy(c).start()

    tables = [
        pltpu.make_async_copy(tcol_hbm, tcol, table_sem.at[0]),
        pltpu.make_async_copy(text_hbm, text, table_sem.at[1]),
    ]
    for table in tables:
        table.start()

    barrier = pltpu.get_barrier_semaphore()

    def around(distance, size):
        return sorted({distance % size, -distance % size} - {0})

    def along_y(distance):
        return [(slab, member(x, (y + j) % ys, k)) for j in around(distance, ys)]

    def along_x(distance):
        return [(slab, member((x + j) % xs, y, k)) for j in around(distance, xs)]

    def along_z(distance):
        return [((slab + j) % zs, swap) for j in around(distance, zs)]

    rounds = [
        along_x(1) + along_y(1) + along_z(1),
        along_y(2) + along_z(2),
        along_z(4),
    ]

    def tell(sem, peers):
        for where in peers:
            pl.semaphore_signal(sem, inc=1, device_id=where, device_id_type=MESH)

    def tell_round(n):
        tell(known.at[n], rounds[n])

    def await_round(n):
        if rounds[n]:
            pl.semaphore_wait(known.at[n], len(rounds[n]))

    neighbours = [next_id, prev_id] + rounds[0]
    tell(barrier, neighbours)
    pl.semaphore_wait(barrier, len(neighbours))

    def send_halo(c):
        own_copy(c).wait()
        to_next(c).start()
        to_prev(c).start()

    looped(0, min(AHEAD, chunks))(send_halo)
    tell_round(0)
    await_round(0)
    tell_round(1)

    sub = lax.broadcasted_iota(jnp.int32, (8, LANES), 0)
    sub3 = lax.broadcasted_iota(jnp.int32, (ys, 8, LANES), 1)
    for table in tables:
        table.wait()
    ext = [text[n] * (DEPTH_SCALE / (layers * zs * members)) for n in range(8)]
    colour = [[tcol[ch, n] for n in range(8)] for ch in range(3)]

    def compute(c):
        r0 = (c % xs) * rows
        col = pl.multiple_of((c // xs) * LANES, LANES)

        @looped(0, ys // 2)
        def _(yh):
            at = (pl.ds(pl.multiple_of(r0 + yh * 8, 8), 8), pl.ds(col, LANES))
            rho = [r[(0, i) + at] for r in (low, own, high) for i in range(layers)]
            mom = [r[(1, i) + at] for r in (low, own, high) for i in range(layers)]
            for step in range(STEPS):
                rho, mom = sweep_step(rho, mom, step == STEPS - 1)
            before = None
            total = [None] * 3
            for i in range(layers):
                dens[(i,) + at] = rho[i]
                m = mat[(i,) + at]
                bits = [(m & b) != 0 for b in (1, 2, 4)]
                through = jnp.exp(-(choose(bits, ext) * rho[i]))
                weight = 1.0 - through
                if before is not None:
                    weight = before * weight
                before = through if before is None else before * through
                for ch in range(3):
                    term = weight * choose(bits, colour[ch])
                    total[ch] = term if total[ch] is None else total[ch] + term
            a = total + [before]
            top = sub < 4
            b = [None] * 4
            for p in range(2):
                b[p] = jnp.where(top, a[p], pltpu.roll(a[p + 2], 4, 0))
                b[p + 2] = jnp.where(top, pltpu.roll(a[p], 4, 0), a[p + 2])
            even = (sub & 2) == 0
            for q in range(2):
                first, second = b[2 * q], b[2 * q + 1]
                part[c, 0, yh * 2 + q] = jnp.where(even, first, pltpu.roll(second, 2, 0))
                part[c, 1, yh * 2 + q] = jnp.where(even, pltpu.roll(first, 6, 0), second)

    def y_copy(c, j):
        other = (y + j) % ys
        return remote(ysrc.at[c, other], ybuf.at[c, y], y_send.at[c], y_recv.at[c], (slab, member(x, other, k)))

    def x_copy(c):
        return remote(xsrc.at[c], xbuf.at[c // xs, x], x_send.at[c], x_recv.at[c // xs], (slab, member(c % xs, y, k)))

    def z_copy(h, j):
        other = (slab + j) % zs
        return remote(zsrc.at[h], zbuf.at[h, slab], z_send.at[h], z_recv.at[h], (other, swap))

    def arrived(ref, sem):
        pltpu.make_async_copy(ref, ref, sem).wait()

    def first_stage(c):
        low_wait = pltpu.make_async_copy(window(low, c), window(low, c), low_recv.at[c])
        low_wait.wait()
        high_wait = pltpu.make_async_copy(window(high, c), window(high, c), high_recv.at[c])
        high_wait.wait()
        mat_copy(c).wait()
        compute(c)
        to_core(c).start()

    def core_stage(c):
        to_core(c).wait_recv()
        mine, theirs = part[c, k], crecv[c]
        is_first = k == 0
        front = jnp.where(is_first, mine, theirs)
        back = jnp.where(is_first, theirs, mine)
        both = over([front, back], sub3)
        ysrc[c] = both
        ybuf[c, y] = ysrc[c, y]
        for j in range(1, ys):
            y_copy(c, j).start()

    def y_stage(c):
        arrived(ybuf.at[c, pl.ds(0, ys - 1)], y_recv.at[c])
        done = over([ybuf[c, i] for i in range(ys)], sub)

        @pl.when(x == c % xs)
        def _():
            xbuf[c // xs, x] = done

        @pl.when(x != c % xs)
        def _():
            xsrc[c] = done
            x_copy(c).start()

    def x_stage(h):
        arrived(xbuf.at[h, pl.ds(0, xs - 1)], x_recv.at[h])
        done = over([xbuf[h, i] for i in range(xs)], sub)
        zsrc[h] = done
        zbuf[h, slab] = done
        for j in range(1, zs):
            z_copy(h, j).start()

    def z_stage(h):
        arrived(zbuf.at[h, pl.ds(0, zs - 1)], z_recv.at[h])
        done = over([zbuf[h, i] for i in range(zs)], sub)
        done = jnp.where(sub < 6, done, 1.0 - done)
        for row in range(2):
            for ch in range(4):
                at = row * halves * LANES + h * LANES
                image[ch : ch + 1, at : at + LANES] = done[2 * ch + row : 2 * ch + row + 1, :]

    @looped(0, chunks + LAG_C + LAG_Y + LAG_X)
    def _(t):
        @pl.when(t < chunks)
        def _():
            first_stage(t)

        if AHEAD < chunks:
            @pl.when(t + AHEAD < chunks)
            def _():
                send_halo(t + AHEAD)

        @pl.when(t == 1)
        def _():
            await_round(1)
            tell_round(2)

        @pl.when(t == 3)
        def _():
            await_round(2)

        @pl.when((t >= LAG_C) & (t < chunks + LAG_C))
        def _():
            core_stage(t - LAG_C)

        ty = t - LAG_C - LAG_Y

        @pl.when((ty >= 0) & (ty < chunks))
        def _():
            y_stage(ty)

        tx = ty - LAG_X

        @pl.when((tx >= 0) & (tx < chunks) & (x == tx % xs))
        def _():
            x_stage(tx // xs)

    for h in range(halves):
        z_stage(h)

    @looped(0, chunks)
    def _(c):
        to_next(c).wait_send()
        to_prev(c).wait_send()
        to_core(c).wait_send()
        arrived(ybuf.at[c, pl.ds(0, ys - 1)], y_send.at[c])

        @pl.when(x != c % xs)
        def _():
            x_copy(c).wait_send()

    for h in range(halves):
        arrived(zbuf.at[h, pl.ds(0, zs - 1)], z_send.at[h])


def per_device(sizes, fluid_state, material, table_colour, table_extinction):
    zs, xs, ys = sizes
    _, layers, height, width = fluid_state.shape
    chunks = 2 * xs
    f32 = jnp.float32
    dma = pltpu.SemaphoreType.DMA
    hbm = pl.BlockSpec(memory_space=pltpu.HBM)
    vmem = pl.BlockSpec(memory_space=pltpu.VMEM)
    density, image = pl.pallas_call(
        functools.partial(kernel, sizes),
        out_shape=(
            jax.ShapeDtypeStruct((layers, height, width), f32),
            jax.ShapeDtypeStruct((4, 4 * LANES), f32),
        ),
        in_specs=[hbm] * 4,
        out_specs=(vmem, vmem),
        scratch_shapes=[
            pltpu.VMEM(fluid_state.shape, f32),
            pltpu.VMEM(fluid_state.shape, f32),
            pltpu.VMEM(fluid_state.shape, f32),
            pltpu.VMEM(material.shape, jnp.int32),
            pltpu.SMEM(table_colour.shape, f32),
            pltpu.SMEM(table_extinction.shape, f32),
            pltpu.VMEM((chunks, 2, ys, 8, LANES), f32),
            pltpu.VMEM((chunks, ys, 8, LANES), f32),
            pltpu.VMEM((chunks, ys, 8, LANES), f32),
            pltpu.VMEM((chunks, ys, 8, LANES), f32),
            pltpu.VMEM((chunks, 8, LANES), f32),
            pltpu.VMEM((2, xs, 8, LANES), f32),
            pltpu.VMEM((2, 8, LANES), f32),
            pltpu.VMEM((2, zs, 8, LANES), f32),
        ]
        + [dma((chunks,))] * 11
        + [dma((2,)), dma((2,)), dma((2,)), dma((2,)), pltpu.SemaphoreType.REGULAR((3,))],
        compiler_params=pltpu.CompilerParams(
            collective_id=0, has_side_effects=True, vmem_limit_bytes=40000000
        ),
        name="sweep_render",
    )(*[pltpu.with_memory_space_constraint(a, pltpu.HBM) for a in (fluid_state, material, table_colour, table_extinction)])
    return density, image


def solution(mesh):
    slabs, members = mesh.shape["slab"], mesh.shape["swap"]
    sizes = (slabs, XS, members // (2 * XS))
    return jax.shard_map(
        functools.partial(per_device, sizes),
        mesh=mesh,
        in_specs=(P(None, ("slab", "swap"), None, None), P(("slab", "swap"), None, None), P(), P()),
        out_specs=(P(("slab", "swap"), None, None), P(None, "swap")),
        check_vma=False,
    )
```

```python
import functools

import jax
import jax.numpy as jnp
from jax import lax
from jax.experimental import pallas as pl
from jax.experimental.pallas import tpu as pltpu
from jax.sharding import PartitionSpec as P

MESH = pl.DeviceIdType.MESH
COURANT = 0.4
DEPTH_SCALE = 2.5
STEPS = 4
LANES = 128
XS = 4
AHEAD = 8
LAG_Y = 8


def sweep_step(rho, mom, last):
    count = len(rho)
    vel = [m / r for m, r in zip(mom, rho)]
    speed = [jnp.abs(v) for v in vel]
    flux = [m * v + r for m, v, r in zip(mom, vel, rho)]
    face_rho, face_mom = [], []
    for i in range(count - 1):
        a = jnp.maximum(speed[i], speed[i + 1]) + 1.0
        face_rho.append((mom[i] + mom[i + 1]) - a * (rho[i + 1] - rho[i]))
        if not last:
            face_mom.append((flux[i] + flux[i + 1]) - a * (mom[i + 1] - mom[i]))
    half = 0.5 * COURANT
    new_rho = [rho[i] - half * (face_rho[i] - face_rho[i - 1]) for i in range(1, count - 1)]
    new_mom = None
    if not last:
        new_mom = [mom[i] - half * (face_mom[i] - face_mom[i - 1]) for i in range(1, count - 1)]
    return new_rho, new_mom


def choose(bits, values):
    level = list(values)
    for bit in bits:
        level = [jnp.where(bit, level[2 * i + 1], level[2 * i]) for i in range(len(level) // 2)]
    return level[0]


def through_everywhere(tile, sub):
    axis = tile.ndim - 2
    only = jnp.where(sub >= 6, tile, 0.0)
    only = only + pltpu.roll(only, 4, axis)
    return only + pltpu.roll(only, 2, axis)


def over(tiles, sub):
    through = [through_everywhere(t, sub) for t in tiles]
    total = tiles[0]
    before = through[0]
    for tile, t in zip(tiles[1:], through[1:]):
        total = total + before * tile
        before = before * t
    return jnp.where(sub < 6, total, before)


def kernel(
    sizes, fluid, material, tcol_hbm, text_hbm, dens, image,
    own, low, high, mat, tcol, text, part, crecv, psrc, pbuf, zsrc, zbuf,
    own_sem, mat_sem, low_recv, high_recv, next_send, prev_send,
    core_send, core_recv, plane_send, plane_recv, z_send, z_recv, table_sem, known,
):
    zs, xs, ys = sizes
    halves = 2
    chunks = halves * xs
    layers = fluid.shape[1]
    rows = 4 * ys
    slab = lax.axis_index("slab")
    swap = lax.axis_index("swap")
    members = 2 * xs * ys
    x = swap // (2 * ys)
    y = (swap // 2) % ys
    k = swap % 2

    def member(xx, yy, kk):
        return (xx * ys + yy) * 2 + kk

    place = slab * members + swap
    after = (place + 1) % (zs * members)
    ahead = (place + zs * members - 1) % (zs * members)
    next_id = (after // members, after % members)
    prev_id = (ahead // members, ahead % members)
    partner = (slab, member(x, y, 1 - k))

    def window(ref, c):
        r = pl.multiple_of((c % xs) * rows, rows)
        col = pl.multiple_of((c // xs) * LANES, LANES)
        where = (pl.ds(r, rows), pl.ds(col, LANES))
        lead = (slice(None),) * (len(ref.shape) - 2)
        return ref.at[lead + where]

    def own_copy(c):
        return pltpu.make_async_copy(window(fluid, c), window(own, c), own_sem.at[c])

    def mat_copy(c):
        return pltpu.make_async_copy(window(material, c), window(mat, c), mat_sem.at[c])

    def remote(src, dst, send, recv, where):
        return pltpu.make_async_remote_copy(
            src_ref=src, dst_ref=dst, send_sem=send, recv_sem=recv, device_id=where, device_id_type=MESH
        )

    def to_next(c):
        return remote(window(own, c), window(low, c), next_send.at[c], low_recv.at[c], next_id)

    def to_prev(c):
        return remote(window(own, c), window(high, c), prev_send.at[c], high_recv.at[c], prev_id)

    def to_core(c):
        return remote(part.at[c, 1 - k], crecv.at[c], core_send.at[c], core_recv.at[c], partner)

    def looped(lo, hi):
        def wrap(body):
            lax.fori_loop(lo, hi, lambda i, _: (body(i), 0)[1], 0)
        return wrap

    barrier = pltpu.get_barrier_semaphore()

    def around(distance, size):
        return sorted({distance % size, -distance % size} - {0})

    def along_y(distance):
        return [(slab, member(x, (y + j) % ys, k)) for j in around(distance, ys)]

    def along_x(distance):
        return [(slab, member((x + j) % xs, y, k)) for j in around(distance, xs)]

    def along_z(distance):
        return [((slab + j) % zs, swap) for j in around(distance, zs)]

    rounds = [
        along_x(1) + along_y(1) + along_z(1),
        along_y(2) + along_z(2),
        along_z(4) + along_x(1) + along_x(2),
    ]

    def far_first(size):
        return sorted(range(1, size), key=lambda j: (-min(j, size - j), j))

    def tell(sem, peers):
        for where in peers:
            pl.semaphore_signal(sem, inc=1, device_id=where, device_id_type=MESH)

    def tell_round(n):
        tell(known.at[n], rounds[n])

    def await_round(n):
        if rounds[n]:
            pl.semaphore_wait(known.at[n], len(rounds[n]))

    neighbours = [next_id, prev_id] + rounds[0]
    tell(barrier, neighbours)
    @looped(0, chunks)
    def _(c):
        own_copy(c).start()

    pl.semaphore_wait(barrier, len(neighbours))

    def send_halo(c):
        own_copy(c).wait()
        to_next(c).start()
        to_prev(c).start()

    looped(0, min(AHEAD, chunks))(send_halo)
    tell_round(0)

    @looped(0, chunks)
    def _(c):
        mat_copy(c).start()

    tables = [
        pltpu.make_async_copy(tcol_hbm, tcol, table_sem.at[0]),
        pltpu.make_async_copy(text_hbm, text, table_sem.at[1]),
    ]
    for table in tables:
        table.start()

    await_round(0)
    tell_round(1)

    sub = lax.broadcasted_iota(jnp.int32, (8, LANES), 0)
    sub3 = lax.broadcasted_iota(jnp.int32, (ys, 8, LANES), 1)
    for table in tables:
        table.wait()
    ext = [text[n] * (DEPTH_SCALE / (layers * zs * members)) for n in range(8)]
    colour = [[tcol[ch, n] for n in range(8)] for ch in range(3)]

    def compute(c):
        r0 = (c % xs) * rows
        col = pl.multiple_of((c // xs) * LANES, LANES)

        @looped(0, ys // 2)
        def _(yh):
            at = (pl.ds(pl.multiple_of(r0 + yh * 8, 8), 8), pl.ds(col, LANES))
            rho = [r[(0, i) + at] for r in (low, own, high) for i in range(layers)]
            mom = [r[(1, i) + at] for r in (low, own, high) for i in range(layers)]
            for step in range(STEPS):
                rho, mom = sweep_step(rho, mom, step == STEPS - 1)
            before = None
            total = [None] * 3
            for i in range(layers):
                dens[(i,) + at] = rho[i]
                m = mat[(i,) + at]
                bits = [(m & b) != 0 for b in (1, 2, 4)]
                through = jnp.exp(-(choose(bits, ext) * rho[i]))
                weight = 1.0 - through
                if before is not None:
                    weight = before * weight
                before = through if before is None else before * through
                for ch in range(3):
                    term = weight * choose(bits, colour[ch])
                    total[ch] = term if total[ch] is None else total[ch] + term
            a = total + [before]
            top = sub < 4
            b = [None] * 4
            for p in range(2):
                b[p] = jnp.where(top, a[p], pltpu.roll(a[p + 2], 4, 0))
                b[p + 2] = jnp.where(top, pltpu.roll(a[p], 4, 0), a[p + 2])
            even = (sub & 2) == 0
            for q in range(2):
                first, second = b[2 * q], b[2 * q + 1]
                part[c, 0, yh * 2 + q] = jnp.where(even, first, pltpu.roll(second, 2, 0))
                part[c, 1, yh * 2 + q] = jnp.where(even, pltpu.roll(first, 6, 0), second)

    def plane_copy(c, j):
        other = (y + j) % ys
        return remote(
            psrc.at[c, other], pbuf.at[c // xs, x * ys + y], plane_send.at[c], plane_recv.at[c // xs],
            (slab, member(c % xs, other, k)),
        )

    def z_copy(h, j):
        other = (slab + j) % zs
        return remote(zsrc.at[h], zbuf.at[h, slab], z_send.at[h], z_recv.at[h], (other, swap))

    def arrived(ref, sem):
        pltpu.make_async_copy(ref, ref, sem).wait()

    def first_stage(c):
        low_wait = pltpu.make_async_copy(window(low, c), window(low, c), low_recv.at[c])
        low_wait.wait()
        high_wait = pltpu.make_async_copy(window(high, c), window(high, c), high_recv.at[c])
        high_wait.wait()
        mat_copy(c).wait()
        compute(c)
        to_core(c).start()

    def core_stage(c):
        to_core(c).wait_recv()
        mine, theirs = part[c, k], crecv[c]
        is_first = k == 0
        front = jnp.where(is_first, mine, theirs)
        back = jnp.where(is_first, theirs, mine)
        both = over([front, back], sub3)
        psrc[c] = both
        for j in far_first(ys):
            plane_copy(c, j).start()

        @pl.when(x == c % xs)
        def _():
            pbuf[c // xs, x * ys + y] = psrc[c, y]

        @pl.when(x != c % xs)
        def _():
            plane_copy(c, 0).start()

    def plane_stage(h):
        arrived(pbuf.at[h, pl.ds(0, xs * ys - 1)], plane_recv.at[h])
        done = over([pbuf[h, i] for i in range(xs * ys)], sub)
        zsrc[h] = done
        zbuf[h, slab] = done
        for j in far_first(zs):
            z_copy(h, j).start()

    def z_stage(h):
        arrived(zbuf.at[h, pl.ds(0, zs - 1)], z_recv.at[h])
        done = over([zbuf[h, i] for i in range(zs)], sub)
        done = jnp.where(sub < 6, done, 1.0 - done)
        for row in range(2):
            for ch in range(4):
                at = row * halves * LANES + h * LANES
                image[ch : ch + 1, at : at + LANES] = done[2 * ch + row : 2 * ch + row + 1, :]

    @looped(0, chunks + 1 + LAG_Y)
    def _(t):
        @pl.when(t < chunks)
        def _():
            first_stage(t)

        if AHEAD < chunks:
            @pl.when(t + AHEAD < chunks)
            def _():
                send_halo(t + AHEAD)

        @pl.when(t == 0)
        def _():
            await_round(1)
            tell_round(2)

        @pl.when(t == 1)
        def _():
            await_round(2)

        @pl.when((t >= 1) & (t < chunks + 1))
        def _():
            core_stage(t - 1)

        ty = t - 1 - LAG_Y

        @pl.when((ty >= 0) & (ty < chunks) & (x == ty % xs))
        def _():
            plane_stage(ty // xs)

    for h in range(halves):
        z_stage(h)

    @looped(0, chunks)
    def _(c):
        to_next(c).wait_send()
        to_prev(c).wait_send()
        to_core(c).wait_send()

        @pl.when(x == c % xs)
        def _():
            arrived(pbuf.at[0, pl.ds(0, ys - 1)], plane_send.at[c])

        @pl.when(x != c % xs)
        def _():
            arrived(pbuf.at[0, pl.ds(0, ys)], plane_send.at[c])

    for h in range(halves):
        arrived(zbuf.at[h, pl.ds(0, zs - 1)], z_send.at[h])


def put(dens, image, dens_out, image_out, sems):
    copies = [
        pltpu.make_async_copy(dens, dens_out, sems.at[0]),
        pltpu.make_async_copy(image, image_out, sems.at[1]),
    ]
    for copy in copies:
        copy.start()
    for copy in copies:
        copy.wait()


def per_device(sizes, fluid_state, material, table_colour, table_extinction):
    zs, xs, ys = sizes
    _, layers, height, width = fluid_state.shape
    chunks = 2 * xs
    f32 = jnp.float32
    dma = pltpu.SemaphoreType.DMA
    hbm = pl.BlockSpec(memory_space=pltpu.HBM)
    vmem = pl.BlockSpec(memory_space=pltpu.VMEM)
    density, image = pl.pallas_call(
        functools.partial(kernel, sizes),
        out_shape=(
            jax.ShapeDtypeStruct((layers, height, width), f32),
            jax.ShapeDtypeStruct((4, 4 * LANES), f32),
        ),
        in_specs=[hbm] * 4,
        out_specs=(vmem, vmem),
        scratch_shapes=[
            pltpu.VMEM(fluid_state.shape, f32),
            pltpu.VMEM(fluid_state.shape, f32),
            pltpu.VMEM(fluid_state.shape, f32),
            pltpu.VMEM(material.shape, jnp.int32),
            pltpu.SMEM(table_colour.shape, f32),
            pltpu.SMEM(table_extinction.shape, f32),
            pltpu.VMEM((chunks, 2, ys, 8, LANES), f32),
            pltpu.VMEM((chunks, ys, 8, LANES), f32),
            pltpu.VMEM((chunks, ys, 8, LANES), f32),
            pltpu.VMEM((2, xs * ys, 8, LANES), f32),
            pltpu.VMEM((2, 8, LANES), f32),
            pltpu.VMEM((2, zs, 8, LANES), f32),
        ]
        + [dma((chunks,))] * 9
        + [dma((2,))] * 4
        + [pltpu.SemaphoreType.REGULAR((3,))],
        compiler_params=pltpu.CompilerParams(
            collective_id=0, has_side_effects=True, vmem_limit_bytes=40000000
        ),
        name="sweep_render",
    )(*[pltpu.with_memory_space_constraint(a, pltpu.HBM) for a in (fluid_state, material, table_colour, table_extinction)])
    return pl.pallas_call(
        put,
        out_shape=(pltpu.HBM(density.shape, f32), pltpu.HBM(image.shape, f32)),
        in_specs=[vmem, vmem],
        out_specs=(hbm, hbm),
        scratch_shapes=[dma((2,))],
        name="put",
    )(*[pltpu.with_memory_space_constraint(a, pltpu.VMEM) for a in (density, image)])


def solution(mesh):
    slabs, members = mesh.shape["slab"], mesh.shape["swap"]
    sizes = (slabs, XS, members // (2 * XS))
    return jax.shard_map(
        functools.partial(per_device, sizes),
        mesh=mesh,
        in_specs=(P(None, ("slab", "swap"), None, None), P(("slab", "swap"), None, None), P(), P()),
        out_specs=(P(("slab", "swap"), None, None), P(None, "swap")),
        check_vma=False,
    )
```

```python
import functools

import jax
import jax.numpy as jnp
from jax import lax
from jax.experimental import pallas as pl
from jax.experimental.pallas import tpu as pltpu
from jax.sharding import PartitionSpec as P

MESH = pl.DeviceIdType.MESH
COURANT = 0.4
DEPTH_SCALE = 2.5
STEPS = 4
LANES = 128
XS = 4
AHEAD = 8
LAG_Y = 8


def sweep_step(rho, mom, last):
    count = len(rho)
    vel = [m / r for m, r in zip(mom, rho)]
    speed = [jnp.abs(v) for v in vel]
    flux = [m * v + r for m, v, r in zip(mom, vel, rho)]
    face_rho, face_mom = [], []
    for i in range(count - 1):
        a = jnp.maximum(speed[i], speed[i + 1]) + 1.0
        face_rho.append((mom[i] + mom[i + 1]) - a * (rho[i + 1] - rho[i]))
        if not last:
            face_mom.append((flux[i] + flux[i + 1]) - a * (mom[i + 1] - mom[i]))
    half = 0.5 * COURANT
    new_rho = [rho[i] - half * (face_rho[i] - face_rho[i - 1]) for i in range(1, count - 1)]
    new_mom = None
    if not last:
        new_mom = [mom[i] - half * (face_mom[i] - face_mom[i - 1]) for i in range(1, count - 1)]
    return new_rho, new_mom


def choose(bits, values):
    level = list(values)
    for bit in bits:
        level = [jnp.where(bit, level[2 * i + 1], level[2 * i]) for i in range(len(level) // 2)]
    return level[0]


def through_everywhere(tile, sub):
    axis = tile.ndim - 2
    only = jnp.where(sub >= 6, tile, 0.0)
    only = only + pltpu.roll(only, 4, axis)
    return only + pltpu.roll(only, 2, axis)


def over(tiles, sub):
    through = [through_everywhere(t, sub) for t in tiles]
    total = tiles[0]
    before = through[0]
    for tile, t in zip(tiles[1:], through[1:]):
        total = total + before * tile
        before = before * t
    return jnp.where(sub < 6, total, before)


def kernel(
    sizes, fluid, material, tcol_hbm, text_hbm, dens, image,
    own, low, high, mat, tcol, text, part, crecv, psrc, pbuf, zsrc, zbuf,
    own_sem, mat_sem, low_recv, high_recv, next_send, prev_send,
    core_send, core_recv, plane_send, plane_recv, z_send, z_recv, table_sem, known,
):
    zs, xs, ys = sizes
    halves = 2
    chunks = halves * xs
    layers = fluid.shape[1]
    rows = 4 * ys
    slab = lax.axis_index("slab")
    swap = lax.axis_index("swap")
    members = 2 * xs * ys
    x = swap // (2 * ys)
    y = (swap // 2) % ys
    k = swap % 2

    def member(xx, yy, kk):
        return (xx * ys + yy) * 2 + kk

    place = slab * members + swap
    after = (place + 1) % (zs * members)
    ahead = (place + zs * members - 1) % (zs * members)
    next_id = (after // members, after % members)
    prev_id = (ahead // members, ahead % members)
    partner = (slab, member(x, y, 1 - k))

    def window(ref, c):
        r = pl.multiple_of((c % xs) * rows, rows)
        col = pl.multiple_of((c // xs) * LANES, LANES)
        where = (pl.ds(r, rows), pl.ds(col, LANES))
        lead = (slice(None),) * (len(ref.shape) - 2)
        return ref.at[lead + where]

    def own_copy(c):
        return pltpu.make_async_copy(window(fluid, c), window(own, c), own_sem.at[c])

    def mat_copy(c):
        return pltpu.make_async_copy(window(material, c), window(mat, c), mat_sem.at[c])

    def remote(src, dst, send, recv, where):
        return pltpu.make_async_remote_copy(
            src_ref=src, dst_ref=dst, send_sem=send, recv_sem=recv, device_id=where, device_id_type=MESH
        )

    def to_next(c):
        return remote(window(own, c), window(low, c), next_send.at[c], low_recv.at[c], next_id)

    def to_prev(c):
        return remote(window(own, c), window(high, c), prev_send.at[c], high_recv.at[c], prev_id)

    def to_core(c):
        return remote(part.at[c, 1 - k], crecv.at[c], core_send.at[c], core_recv.at[c], partner)

    def looped(lo, hi):
        def wrap(body):
            lax.fori_loop(lo, hi, lambda i, _: (body(i), 0)[1], 0)
        return wrap

    barrier = pltpu.get_barrier_semaphore()

    def around(distance, size):
        return sorted({distance % size, -distance % size} - {0})

    def along_y(distance):
        return [(slab, member(x, (y + j) % ys, k)) for j in around(distance, ys)]

    def along_x(distance):
        return [(slab, member((x + j) % xs, y, k)) for j in around(distance, xs)]

    def along_z(distance):
        return [((slab + j) % zs, swap) for j in around(distance, zs)]

    rounds = [
        along_x(1) + along_y(1) + along_z(1),
        along_y(2) + along_z(2),
        along_z(4) + along_x(1) + along_x(2),
    ]

    def far_first(size):
        return sorted(range(1, size), key=lambda j: (-min(j, size - j), j))

    def tell(sem, peers):
        for where in peers:
            pl.semaphore_signal(sem, inc=1, device_id=where, device_id_type=MESH)

    def tell_round(n):
        tell(known.at[n], rounds[n])

    def await_round(n):
        if rounds[n]:
            pl.semaphore_wait(known.at[n], len(rounds[n]))

    neighbours = [next_id, prev_id] + rounds[0]
    tell(barrier, neighbours)
    @looped(0, chunks)
    def _(c):
        own_copy(c).start()

    pl.semaphore_wait(barrier, len(neighbours))

    def send_halo(c):
        own_copy(c).wait()
        to_next(c).start()
        to_prev(c).start()

    looped(0, min(AHEAD, chunks))(send_halo)
    tell_round(0)

    @looped(0, chunks)
    def _(c):
        mat_copy(c).start()

    tables = [
        pltpu.make_async_copy(tcol_hbm, tcol, table_sem.at[0]),
        pltpu.make_async_copy(text_hbm, text, table_sem.at[1]),
    ]
    for table in tables:
        table.start()

    await_round(0)
    tell_round(1)

    sub = lax.broadcasted_iota(jnp.int32, (8, LANES), 0)
    sub3 = lax.broadcasted_iota(jnp.int32, (ys, 8, LANES), 1)
    for table in tables:
        table.wait()
    ext = [text[n] * (DEPTH_SCALE / (layers * zs * members)) for n in range(8)]
    colour = [[tcol[ch, n] for n in range(8)] for ch in range(3)]

    def compute(c):
        r0 = (c % xs) * rows
        col = pl.multiple_of((c // xs) * LANES, LANES)

        @looped(0, ys // 2)
        def _(yh):
            at = (pl.ds(pl.multiple_of(r0 + yh * 8, 8), 8), pl.ds(col, LANES))
            rho = [r[(0, i) + at] for r in (low, own, high) for i in range(layers)]
            mom = [r[(1, i) + at] for r in (low, own, high) for i in range(layers)]
            for step in range(STEPS):
                rho, mom = sweep_step(rho, mom, step == STEPS - 1)
            before = None
            total = [None] * 3
            for i in range(layers):
                dens[(i,) + at] = rho[i]
                m = mat[(i,) + at]
                bits = [(m & b) != 0 for b in (1, 2, 4)]
                through = jnp.exp(-(choose(bits, ext) * rho[i]))
                weight = 1.0 - through
                if before is not None:
                    weight = before * weight
                before = through if before is None else before * through
                for ch in range(3):
                    term = weight * choose(bits, colour[ch])
                    total[ch] = term if total[ch] is None else total[ch] + term
            a = total + [before]
            top = sub < 4
            b = [None] * 4
            for p in range(2):
                b[p] = jnp.where(top, a[p], pltpu.roll(a[p + 2], 4, 0))
                b[p + 2] = jnp.where(top, pltpu.roll(a[p], 4, 0), a[p + 2])
            even = (sub & 2) == 0
            for q in range(2):
                first, second = b[2 * q], b[2 * q + 1]
                part[c, 0, yh * 2 + q] = jnp.where(even, first, pltpu.roll(second, 2, 0))
                part[c, 1, yh * 2 + q] = jnp.where(even, pltpu.roll(first, 6, 0), second)

    def plane_copy(c, j):
        other = (y + j) % ys
        return remote(
            psrc.at[c, other], pbuf.at[c // xs, x * ys + y], plane_send.at[c], plane_recv.at[c // xs],
            (slab, member(c % xs, other, k)),
        )

    def z_copy(h, j):
        other = (slab + j) % zs
        return remote(zsrc.at[h], zbuf.at[h, slab], z_send.at[h], z_recv.at[h], (other, swap))

    def arrived(ref, sem):
        pltpu.make_async_copy(ref, ref, sem).wait()

    def first_stage(c):
        low_wait = pltpu.make_async_copy(window(low, c), window(low, c), low_recv.at[c])
        low_wait.wait()
        high_wait = pltpu.make_async_copy(window(high, c), window(high, c), high_recv.at[c])
        high_wait.wait()
        mat_copy(c).wait()
        compute(c)
        to_core(c).start()

    def core_stage(c):
        to_core(c).wait_recv()
        mine, theirs = part[c, k], crecv[c]
        is_first = k == 0
        front = jnp.where(is_first, mine, theirs)
        back = jnp.where(is_first, theirs, mine)
        both = over([front, back], sub3)
        psrc[c] = both
        for j in far_first(ys):
            plane_copy(c, j).start()

        @pl.when(x == c % xs)
        def _():
            pbuf[c // xs, x * ys + y] = psrc[c, y]

        @pl.when(x != c % xs)
        def _():
            plane_copy(c, 0).start()

    def plane_stage(h):
        arrived(pbuf.at[h, pl.ds(0, xs * ys - 1)], plane_recv.at[h])
        done = over([pbuf[h, i] for i in range(xs * ys)], sub)
        zsrc[h] = done
        zbuf[h, slab] = done
        for j in far_first(zs):
            z_copy(h, j).start()

    def z_stage(h):
        arrived(zbuf.at[h, pl.ds(0, zs - 1)], z_recv.at[h])
        done = over([zbuf[h, i] for i in range(zs)], sub)
        done = jnp.where(sub < 6, done, 1.0 - done)
        for row in range(2):
            for ch in range(4):
                at = row * halves * LANES + h * LANES
                image[ch : ch + 1, at : at + LANES] = done[2 * ch + row : 2 * ch + row + 1, :]

    @looped(0, chunks + 1 + LAG_Y)
    def _(t):
        @pl.when(t < chunks)
        def _():
            first_stage(t)

        if AHEAD < chunks:
            @pl.when(t + AHEAD < chunks)
            def _():
                send_halo(t + AHEAD)

        @pl.when(t == 0)
        def _():
            await_round(1)
            tell_round(2)

        @pl.when(t == 1)
        def _():
            await_round(2)

        @pl.when((t >= 1) & (t < chunks + 1))
        def _():
            core_stage(t - 1)

        ty = t - 1 - LAG_Y

        @pl.when((ty >= 0) & (ty < chunks) & (x == ty % xs))
        def _():
            plane_stage(ty // xs)

    @looped(0, chunks)
    def _(c):
        to_next(c).wait_send()
        to_prev(c).wait_send()
        to_core(c).wait_send()

        @pl.when(x == c % xs)
        def _():
            arrived(pbuf.at[0, pl.ds(0, ys - 1)], plane_send.at[c])

        @pl.when(x != c % xs)
        def _():
            arrived(pbuf.at[0, pl.ds(0, ys)], plane_send.at[c])

    for h in range(halves):
        z_stage(h)

    for h in range(halves):
        arrived(zbuf.at[h, pl.ds(0, zs - 1)], z_send.at[h])


def put(dens, image, dens_out, image_out, sems):
    copies = [
        pltpu.make_async_copy(dens, dens_out, sems.at[0]),
        pltpu.make_async_copy(image, image_out, sems.at[1]),
    ]
    for copy in copies:
        copy.start()
    for copy in copies:
        copy.wait()


def per_device(sizes, fluid_state, material, table_colour, table_extinction):
    zs, xs, ys = sizes
    _, layers, height, width = fluid_state.shape
    chunks = 2 * xs
    f32 = jnp.float32
    dma = pltpu.SemaphoreType.DMA
    hbm = pl.BlockSpec(memory_space=pltpu.HBM)
    vmem = pl.BlockSpec(memory_space=pltpu.VMEM)
    density, image = pl.pallas_call(
        functools.partial(kernel, sizes),
        out_shape=(
            jax.ShapeDtypeStruct((layers, height, width), f32),
            jax.ShapeDtypeStruct((4, 4 * LANES), f32),
        ),
        in_specs=[hbm] * 4,
        out_specs=(vmem, vmem),
        scratch_shapes=[
            pltpu.VMEM(fluid_state.shape, f32),
            pltpu.VMEM(fluid_state.shape, f32),
            pltpu.VMEM(fluid_state.shape, f32),
            pltpu.VMEM(material.shape, jnp.int32),
            pltpu.SMEM(table_colour.shape, f32),
            pltpu.SMEM(table_extinction.shape, f32),
            pltpu.VMEM((chunks, 2, ys, 8, LANES), f32),
            pltpu.VMEM((chunks, ys, 8, LANES), f32),
            pltpu.VMEM((chunks, ys, 8, LANES), f32),
            pltpu.VMEM((2, xs * ys, 8, LANES), f32),
            pltpu.VMEM((2, 8, LANES), f32),
            pltpu.VMEM((2, zs, 8, LANES), f32),
        ]
        + [dma((chunks,))] * 9
        + [dma((2,))] * 4
        + [pltpu.SemaphoreType.REGULAR((3,))],
        compiler_params=pltpu.CompilerParams(
            collective_id=0, has_side_effects=True, vmem_limit_bytes=40000000
        ),
        name="sweep_render",
    )(*[pltpu.with_memory_space_constraint(a, pltpu.HBM) for a in (fluid_state, material, table_colour, table_extinction)])
    return pl.pallas_call(
        put,
        out_shape=(pltpu.HBM(density.shape, f32), pltpu.HBM(image.shape, f32)),
        in_specs=[vmem, vmem],
        out_specs=(hbm, hbm),
        scratch_shapes=[dma((2,))],
        name="put",
    )(*[pltpu.with_memory_space_constraint(a, pltpu.VMEM) for a in (density, image)])


def solution(mesh):
    slabs, members = mesh.shape["slab"], mesh.shape["swap"]
    sizes = (slabs, XS, members // (2 * XS))
    return jax.shard_map(
        functools.partial(per_device, sizes),
        mesh=mesh,
        in_specs=(P(None, ("slab", "swap"), None, None), P(("slab", "swap"), None, None), P(), P()),
        out_specs=(P(("slab", "swap"), None, None), P(None, "swap")),
        check_vma=False,
    )
```
